32 devices in a mesh: replica: 8 (over z, y), fsdp: 4 (over x, core).
Axes of the slice: x: 2, y: 2, z: 4, core: 2. Of those that a mesh axis runs over, the one named last changes fastest.
Arguments:
- block_in: bfloat16 [1, 131072, 896], P(None, ('replica', 'fsdp'))
- grad_out: bfloat16 [131072, 896], P(('replica', 'fsdp'))
- w_up: bfloat16 [1, 896, 4864], P(None, 'fsdp')
- w_lin: bfloat16 [1, 896, 4864], P(None, 'fsdp')
- w_down: bfloat16 [1, 4864, 896], P(None, 'fsdp')
Outputs:
- output 1: float32 [1, 896, 4864], P(None, 'fsdp')
- output 2: float32 [1, 896, 4864], P(None, 'fsdp')
- output 3: float32 [1, 4864, 896], P(None, 'fsdp')
- output 4: bfloat16 [131072, 896], P(('replica', 'fsdp'))
All inputs are finite; a program needn't handle non-finite values.
Results may differ from the reference program's by a relative error of at most 0.001.
Values are sent between devices in bfloat16 or wider.
A program may use at most 1 GiB of HBM per device.

```python
import jax
import jax.numpy as jnp
from jax import lax

D = 896
FF = 4864
LAYERS = 1
TOK_DEV = 4096
REPLICA = 8
FSDP = 4
TOKENS = TOK_DEV * REPLICA * FSDP
NUM_BLOCKS = REPLICA * FSDP
NORM_EPS = 1e-5


def setup_inputs(seed: int = 0) -> dict:
    key_list = jax.random.split(jax.random.key(seed), 5)
    block_in = jax.random.normal(key_list[0], (LAYERS, TOKENS, D), jnp.float32).astype(jnp.bfloat16)
    grad_out = jax.random.normal(key_list[1], (TOKENS, D), jnp.float32).astype(jnp.bfloat16)
    w_up = (jax.random.normal(key_list[2], (LAYERS, D, FF), jnp.float32) * D ** -0.5).astype(jnp.bfloat16)
    w_lin = (jax.random.normal(key_list[3], (LAYERS, D, FF), jnp.float32) * D ** -0.5).astype(jnp.bfloat16)
    w_down = (jax.random.normal(key_list[4], (LAYERS, FF, D), jnp.float32) * (0.5 * FF ** -0.5)).astype(jnp.bfloat16)
    return {'block_in': block_in, 'grad_out': grad_out, 'w_up': w_up, 'w_lin': w_lin, 'w_down': w_down}


def layer_grad(h_in, grad_acc, up_w, lin_w, down_w):
    h_f32 = h_in.astype(jnp.float32)
    inv_rms = lax.rsqrt(jnp.mean(h_f32 * h_f32, axis=-1, keepdims=True) + NORM_EPS)
    normed = h_f32 * inv_rms
    normed_b = normed.astype(jnp.bfloat16)
    pre_up = jnp.dot(normed_b, up_w, preferred_element_type=jnp.float32)
    pre_lin = jnp.dot(normed_b, lin_w, preferred_element_type=jnp.float32)
    up_sig = jax.nn.sigmoid(pre_up)
    up_act = pre_up * up_sig
    act_b = (up_act * pre_lin).astype(jnp.bfloat16)
    grad_b = grad_acc.astype(jnp.bfloat16)
    d_act = jnp.dot(grad_b, down_w.T, preferred_element_type=jnp.float32)
    d_up = (d_act * pre_lin * up_sig * (1.0 + pre_up * (1.0 - up_sig))).astype(jnp.bfloat16)
    d_lin = (d_act * up_act).astype(jnp.bfloat16)
    g_down = jnp.dot(act_b.T, grad_b, preferred_element_type=jnp.float32)
    g_up = jnp.dot(normed_b.T, d_up, preferred_element_type=jnp.float32)
    g_lin = jnp.dot(normed_b.T, d_lin, preferred_element_type=jnp.float32)
    d_norm = jnp.dot(d_up, up_w.T, preferred_element_type=jnp.float32) + jnp.dot(d_lin, lin_w.T, preferred_element_type=jnp.float32)
    d_h = inv_rms * (d_norm - normed * jnp.mean(d_norm * normed, axis=-1, keepdims=True))
    return grad_acc + d_h, g_up, g_lin, g_down


def reference(block_in, grad_out, w_up, w_lin, w_down):
    blocks_in = block_in.reshape(LAYERS, NUM_BLOCKS, TOK_DEV, D).transpose(1, 0, 2, 3)
    blocks_grad = grad_out.reshape(NUM_BLOCKS, TOK_DEV, D)

    def block_step(grad_sums, block_xs):
        h_block, g_block = block_xs

        def layer_step(grad_acc, layer_xs):
            h_layer, up_w, lin_w, down_w = layer_xs
            new_grad, g_up, g_lin, g_down = layer_grad(h_layer, grad_acc, up_w, lin_w, down_w)
            return new_grad, (g_up, g_lin, g_down)

        final_grad, layer_grads = lax.scan(layer_step, g_block.astype(jnp.float32), (h_block, w_up, w_lin, w_down), reverse=True)
        new_sums = tuple(old_part + new_part for old_part, new_part in zip(grad_sums, layer_grads))
        return new_sums, final_grad.astype(jnp.bfloat16)

    zero_sums = (jnp.zeros((LAYERS, D, FF), jnp.float32), jnp.zeros((LAYERS, D, FF), jnp.float32), jnp.zeros((LAYERS, FF, D), jnp.float32))
    grad_sums, grad_blocks = lax.scan(block_step, zero_sums, (blocks_in, blocks_grad))
    return grad_sums[0], grad_sums[1], grad_sums[2], grad_blocks.reshape(TOKENS, D)
```

```python
import functools

import jax
import jax.numpy as jnp
from jax import lax
from jax.experimental import pallas as pl
from jax.experimental.pallas import tpu as pltpu
from jax.sharding import PartitionSpec as P

NORM_EPS = 1e-5
LANE = 128
CHUNKS = ((0, 1, 10, 11), (2, 3, 4, 12, 13, 14), (5, 6, 7, 8, 15, 16, 17, 18, 9))
ORDER = sum(CHUNKS, ())
GROUP = 2
TILE = 512
DN_TILE = 512
SPLIT = 3
F32 = jnp.float32
BF16 = jnp.bfloat16


def dot(a, b):
    return lax.dot_general(a, b, (((1,), (0,)), ((), ())), preferred_element_type=F32)


def dot_t(a, b):
    return lax.dot_general(a, b, (((1,), (1,)), ((), ())), preferred_element_type=F32)


def group_kernel(units, core_ref, n_ref, nt_ref, g_ref, gt_ref, *refs):
    blocks, refs = refs[: 8 * units], refs[8 * units :]
    du_ref, dv_ref, send_ref, keep_ref, acc_up, acc_lin, acc_down, flip, up_ref, lin_ref, down_ref = refs[-11:]
    step = pl.program_id(0)

    @pl.when(step == 0)
    def _():
        acc_up[...] = jnp.zeros_like(acc_up)
        acc_lin[...] = jnp.zeros_like(acc_lin)
        acc_down[...] = jnp.zeros_like(acc_down)
        for i in range(2 * units):
            up_ref[:, pl.ds(i * LANE, LANE)] = blocks[i][...]
            lin_ref[:, pl.ds(i * LANE, LANE)] = blocks[2 * units + i][...]
        half = LANE // 2
        for i in range(4 * units):
            down_ref[pl.ds(i * half, half), :] = blocks[4 * units + i][...]

    u = dot(n_ref[...], up_ref[...])
    v = dot(n_ref[...], lin_ref[...])
    da = dot_t(g_ref[...], down_ref[...])
    s = jax.nn.sigmoid(u)
    us = u * s
    a = (us * v).astype(BF16)
    du = (da * v * s * (1.0 + u * (1.0 - s))).astype(BF16)
    dv = (da * us).astype(BF16)
    du_ref[...] = du
    dv_ref[...] = dv
    acc_down[...] += dot(gt_ref[...], a)
    acc_up[...] += dot(nt_ref[...], du)
    acc_lin[...] += dot(nt_ref[...], dv)

    @pl.when(step == pl.num_programs(0) - 1)
    def _():
        core = core_ref[0]
        rows = acc_up.shape[0] // 4
        unit_rows = 6 * rows
        for unit in range(units):
            base = unit * unit_rows
            for x in range(2):
                flip[...] = acc_down[:, pl.ds((2 * unit + x) * LANE, LANE)].T
                for out_ref, owner in ((send_ref, 1 - core), (keep_ref, core)):
                    first = pl.multiple_of((2 * x + owner) * rows, 8)
                    for piece in range(2):
                        cols = pl.ds((2 * unit + piece) * LANE, LANE)
                        out_ref[x, pl.ds(base + piece * rows, rows), :] = acc_up[pl.ds(first, rows), cols]
                        out_ref[x, pl.ds(base + (4 + piece) * rows, rows), :] = acc_lin[pl.ds(first, rows), cols]
                    half = LANE // 2
                    for lane in range(flip.shape[1] // LANE):
                        out_ref[x, pl.ds(base + 2 * rows + lane * half, half), :] = flip[pl.ds(pl.multiple_of(owner * half, 8), half), pl.ds(lane * LANE, LANE)]


def chunk_of(unit):
    for index, chunk in enumerate(CHUNKS):
        if unit in chunk:
            return index, chunk


def col_block(unit, x):
    index, chunk = chunk_of(unit)
    return x * len(chunk) + chunk.index(unit)


def row_block(unit, x, half):
    index, chunk = chunk_of(unit)
    mid = len(ORDER) // 2
    length = sum(2 if other < mid else 1 for other in chunk if other <= mid)
    core = half if unit == mid else int(unit > mid)
    mates = [other for other in chunk if other != mid and (other > mid) == (unit > mid)]
    place = 2 * len(mates) if unit == mid else 2 * mates.index(unit) + half
    return (2 * x + core) * length + place


def group_call(group, offset, token, normed, normed_t, grad, grad_t, ups, lins, downs, d_up, d_lin):
    tokens, dim = normed.shape
    units = len(group)
    width = 2 * LANE * units
    total = 2 * LANE * len(ORDER)
    packed = units * 6 * (dim // 4)
    tok = pl.BlockSpec((TILE, dim), lambda i, c: (i, 0))
    tok_t = pl.BlockSpec((dim, TILE), lambda i, c: (0, i))
    wide = pl.BlockSpec((TILE, width), lambda i, c: (i, offset // units))
    out = pl.BlockSpec((2, packed, LANE), lambda i, c: (0, 0, 0))
    ins = [token, normed, normed_t, grad, grad_t]
    in_specs = [tok, tok_t, tok, tok_t]
    for weights in (ups, lins):
        for unit in group:
            for x in range(2):
                ins.append(weights[chunk_of(unit)[0]])
                in_specs.append(pl.BlockSpec((dim, LANE), lambda i, c, at=col_block(unit, x): (0, at)))
    for unit in group:
        for x in range(2):
            for half in range(2):
                ins.append(downs[chunk_of(unit)[0]])
                in_specs.append(pl.BlockSpec((LANE // 2, dim), lambda i, c, at=row_block(unit, x, half): (at, 0)))
    aliases = {}
    if d_up is not None:
        aliases = {len(ins): 0, len(ins) + 1: 1}
        ins += [d_up, d_lin]
        in_specs += [pl.BlockSpec(memory_space=pl.ANY)] * 2
    return pl.pallas_call(
        functools.partial(group_kernel, units),
        grid_spec=pltpu.PrefetchScalarGridSpec(
            num_scalar_prefetch=1,
            grid=(tokens // TILE,),
            in_specs=in_specs,
            out_specs=[wide, wide, out, out],
            scratch_shapes=[pltpu.VMEM((dim, width), F32)] * 3 + [pltpu.VMEM((LANE, dim), F32)] + [pltpu.VMEM((dim, width), BF16)] * 2 + [pltpu.VMEM((width, dim), BF16)],
        ),
        out_shape=[jax.ShapeDtypeStruct((tokens, total), BF16)] * 2 + [jax.ShapeDtypeStruct((2, packed, LANE), F32)] * 2,
        input_output_aliases=aliases,
        compiler_params=pltpu.CompilerParams(dimension_semantics=('arbitrary',), vmem_limit_bytes=58 * 1024 * 1024),
        cost_estimate=pl.CostEstimate(flops=12 * tokens * dim * width, bytes_accessed=8 * tokens * dim, transcendentals=tokens * width),
        name='group',
    )(*ins)


def advance_kernel(plan, pos_ref, *refs):
    ins, outs = refs[: sum(4 if bit is not None and not gather else 2 for bit, gather in plan)], refs[-sum(1 if gather or bit is None else 2 for bit, gather in plan) :]
    for bit, gather in plan:
        if gather:
            at = pos_ref[bit]
            outs[0][at] = ins[0][...]
            outs[0][1 - at] = ins[1][...]
            ins, outs = ins[2:], outs[1:]
        elif bit is None:
            outs[0][...] = ins[0][...] + ins[1][...]
            ins, outs = ins[2:], outs[1:]
        else:
            outs[0][...] = ins[0][...] + ins[1][...]
            outs[1][...] = ins[2][...] + ins[3][...]
            ins, outs = ins[4:], outs[2:]


def advance_call(pos, plan, pairs):
    ins, in_specs, shapes, out_specs = [pos], [], [], []
    for (bit, gather), (kept, got) in zip(plan, pairs):
        rows = kept.shape[-2] if kept.ndim == 3 else kept.shape[0]
        if gather:
            block = rows // SPLIT
            ins += [kept, got]
            in_specs += [pl.BlockSpec((block, LANE), lambda i, p: (i, 0))] * 2
            shapes.append(jax.ShapeDtypeStruct((2, rows, LANE), F32))
            out_specs.append(pl.BlockSpec((2, block, LANE), lambda i, p: (0, i, 0)))
        elif bit is None:
            block = rows // SPLIT
            ins += [kept, got]
            in_specs += [pl.BlockSpec((block, LANE), lambda i, p: (i, 0))] * 2
            shapes.append(jax.ShapeDtypeStruct((rows, LANE), F32))
            out_specs.append(pl.BlockSpec((block, LANE), lambda i, p: (i, 0)))
        else:
            if kept.ndim == 2:
                rows //= 2
                kept, got = kept.reshape(2, rows, LANE), got.reshape(2, rows, LANE)
            block = rows // SPLIT
            other = pl.BlockSpec((None, block, LANE), lambda i, p, bit=bit: (1 - p[bit], i, 0))
            mine = pl.BlockSpec((None, block, LANE), lambda i, p, bit=bit: (p[bit], i, 0))
            ins += [kept, got, kept, got]
            in_specs += [other, other, mine, mine]
            shapes += [jax.ShapeDtypeStruct((rows, LANE), F32)] * 2
            out_specs += [pl.BlockSpec((block, LANE), lambda i, p: (i, 0))] * 2
    return pl.pallas_call(
        functools.partial(advance_kernel, plan),
        grid_spec=pltpu.PrefetchScalarGridSpec(num_scalar_prefetch=1, grid=(SPLIT,), in_specs=in_specs, out_specs=out_specs),
        out_shape=shapes,
        compiler_params=pltpu.CompilerParams(dimension_semantics=('arbitrary',), vmem_limit_bytes=40 * 1024 * 1024),
        cost_estimate=pl.CostEstimate(flops=10**7, bytes_accessed=2 * 10**7, transcendentals=0),
        name='advance',
    )(*ins)


def unpack_kernel(up_ref, lin_ref, up_out, lin_out):
    units = len(ORDER)
    for index, unit in enumerate(ORDER):
        for x in range(2):
            cols = pl.ds((x * units + unit) * LANE, LANE)
            up_out[:, cols] = up_ref[index, x]
            lin_out[:, cols] = lin_ref[index, x]


def unpack_call(packed):
    units, _, rows, _ = packed.shape
    block = rows // 7
    return pl.pallas_call(
        unpack_kernel,
        grid=(7,),
        in_specs=[pl.BlockSpec((units, 2, block, LANE), lambda i: (0, 0, i, 0)), pl.BlockSpec((units, 2, block, LANE), lambda i: (0, 2, i, 0))],
        out_specs=[pl.BlockSpec((block, 2 * units * LANE), lambda i: (i, 0))] * 2,
        out_shape=[jax.ShapeDtypeStruct((rows, 2 * units * LANE), F32)] * 2,
        compiler_params=pltpu.CompilerParams(dimension_semantics=('arbitrary',)),
        name='unpack',
    )(packed, packed)


def rows_kernel(in_ref, out_ref):
    for lane in range(in_ref.shape[0]):
        out_ref[:, pl.ds(lane * LANE, LANE)] = in_ref[lane]


def rows_call(blocks):
    count, lanes, rows, _ = blocks.shape
    return pl.pallas_call(
        rows_kernel,
        grid=(count,),
        in_specs=[pl.BlockSpec((None, lanes, rows, LANE), lambda i: (i, 0, 0, 0))],
        out_specs=pl.BlockSpec((rows, lanes * LANE), lambda i: (i, 0)),
        out_shape=jax.ShapeDtypeStruct((count * rows, lanes * LANE), F32),
        compiler_params=pltpu.CompilerParams(dimension_semantics=('arbitrary',)),
        name='rows',
    )(blocks)


def input_kernel(token_ref, du_ref, dv_ref, *refs):
    weights, (h_ref, g_ref), (out_ref, acc) = refs[: 4 * len(CHUNKS)], refs[4 * len(CHUNKS) : 4 * len(CHUNKS) + 2], refs[-2:]
    k = pl.program_id(0)

    @pl.when(k == 0)
    def _():
        acc[...] = jnp.zeros_like(acc)

    first = 0
    for index, chunk in enumerate(CHUNKS):

        @pl.when((k >= first) & (k < first + len(chunk)))
        def _(index=index):
            up0, up1, lin0, lin1 = (ref[...] for ref in weights[4 * index : 4 * index + 4])
            acc[...] += dot_t(du_ref[...], jnp.concatenate([up0, up1], axis=1)) + dot_t(dv_ref[...], jnp.concatenate([lin0, lin1], axis=1))

        first += len(chunk)

    @pl.when(k == pl.num_programs(0) - 1)
    def _():
        h = h_ref[...].astype(F32)
        inv = lax.rsqrt(jnp.mean(h * h, axis=-1, keepdims=True) + NORM_EPS)
        y = h * inv
        dn = acc[...]
        d_h = inv * (dn - y * jnp.mean(dn * y, axis=-1, keepdims=True))
        out_ref[...] = (g_ref[...].astype(F32) + d_h).astype(BF16)


def input_call(part, token, d_up, d_lin, ups, lins, h, grad, prev):
    tokens, dim = h.shape
    wide = 2 * LANE
    steps = d_up.shape[1] // wide
    act = pl.BlockSpec((DN_TILE, wide), lambda k, c: (part, k))
    tok = pl.BlockSpec((DN_TILE, dim), lambda k, c: (part, 0))
    ins = [token, d_up, d_lin]
    in_specs = [act, act]
    first = 0
    for index, chunk in enumerate(CHUNKS):
        for weights in (ups, lins):
            for x in range(2):
                ins.append(weights[index])
                in_specs.append(pl.BlockSpec((dim, LANE), lambda k, c, n=len(chunk), at=x * len(chunk), first=first: (0, at + jnp.clip(k - first, 0, n - 1))))
        first += len(chunk)
    ins += [h, grad]
    in_specs += [tok, tok]
    aliases = {}
    if prev is not None:
        aliases = {len(ins): 0}
        ins.append(prev)
        in_specs.append(pl.BlockSpec(memory_space=pl.ANY))
    return pl.pallas_call(
        input_kernel,
        grid_spec=pltpu.PrefetchScalarGridSpec(num_scalar_prefetch=1, grid=(steps,), in_specs=in_specs, out_specs=tok, scratch_shapes=[pltpu.VMEM((DN_TILE, dim), F32)]),
        out_shape=jax.ShapeDtypeStruct((tokens, dim), BF16),
        input_output_aliases=aliases,
        compiler_params=pltpu.CompilerParams(dimension_semantics=('arbitrary',), vmem_limit_bytes=40 * 1024 * 1024),
        cost_estimate=pl.CostEstimate(flops=4 * DN_TILE * dim * d_up.shape[1], bytes_accessed=4 * DN_TILE * d_up.shape[1], transcendentals=0),
        name='input_grad',
    )(*ins)


def solution(mesh):
    tok_spec = P(('replica', 'fsdp'), None)
    act_spec = P(None, ('replica', 'fsdp'), None)
    weight_spec = P(None, 'fsdp', None)
    n_fsdp, n_rep = mesh.shape['fsdp'], mesh.shape['replica']

    def swap(value, axis, bit):
        size = n_fsdp if axis == 'fsdp' else n_rep
        return lax.ppermute(value, axis, [(i, i ^ bit) for i in range(size)])

    def local_step(block_in, grad_out, w_up, w_lin, w_down):
        h = block_in[0]
        dim, ff = h.shape[1], w_up.shape[2]
        n_units = len(ORDER)
        fsdp, rep = lax.axis_index('fsdp'), lax.axis_index('replica')
        core = fsdp % 2
        pos = jnp.stack([core, fsdp // 2, rep % 2, (rep // 2) % 2, rep // 4]).astype(jnp.int32)

        def cut_cols(w, chunk):
            pieces = []
            for x in range(2):
                run = [chunk[0]]
                for unit in chunk[1:] + (-1,):
                    if unit == run[-1] + 1:
                        run.append(unit)
                    else:
                        pieces.append(w[:, (x * n_units + run[0]) * LANE : (x * n_units + run[-1] + 1) * LANE])
                        run = [unit]
            return jnp.concatenate(pieces, axis=1)

        gather = lambda w: lax.all_gather(w, 'fsdp', axis=0, tiled=True)
        half = LANE // 2
        rolled = jnp.concatenate([w_down[0], w_down[0][:half]], axis=0)
        ups, lins, downs = [], [], []
        start = 0
        hold = 0
        for chunk in CHUNKS:
            length = half * len(chunk)
            parts = (cut_cols(w_up[0], chunk), cut_cols(w_lin[0], chunk), lax.dynamic_slice_in_dim(rolled, start + core * half, length, 0))
            start += length
            for out, part in zip((ups, lins, downs), parts):
                out.append(gather(part))

        h_f32 = h.astype(F32)
        inv_rms = lax.rsqrt(jnp.mean(h_f32 * h_f32, axis=-1, keepdims=True) + NORM_EPS)
        normed = (h_f32 * inv_rms).astype(BF16)
        normed_t, grad_t = normed.T, grad_out.T

        groups = []
        for chunk in CHUNKS:
            groups += [chunk[i : i + GROUP] for i in range(0, len(chunk), GROUP)]
        links = (('fsdp', 1), ('fsdp', 2), ('replica', 1), ('replica', 2), ('replica', 4), ('replica', 4), ('replica', 2), ('replica', 1))
        plan_of = ((1, False), (2, False), (3, False), (4, False), (None, False), (4, True), (3, True), (2, True))

        d_up = d_lin = out = None
        parts = h.shape[0] // DN_TILE
        flying, done = [], {}
        slot = part = offset = 0
        while slot < len(groups) or part < parts or flying:
            token, sends = lax.optimization_barrier((pos, [item[2] for item in flying]))
            got = [swap(value, *links[item[1]]) for value, item in zip(sends, flying)]
            fresh = None
            if slot < len(groups):
                d_up, d_lin, send, keep = group_call(groups[slot], offset, token, normed, normed_t, grad_out, grad_t, ups, lins, downs, d_up, d_lin)
                fresh = [slot, 0, send, keep]
                offset += len(groups[slot])
                slot += 1
            elif part < parts:
                out = input_call(part, token, d_up, d_lin, ups, lins, h, grad_out, out)
                part += 1
            if flying:
                plan = tuple(plan_of[item[1]] for item in flying)
                made = list(advance_call(pos, plan, [(item[3], value) for item, value in zip(flying, got)]))
                after = []
                for (bit, joined), item in zip(plan, flying):
                    if joined or bit is None:
                        value = made.pop(0)
                        value = value.reshape(-1, LANE)
                        nxt = [item[0], item[1] + 1, value, value]
                    else:
                        nxt = [item[0], item[1] + 1, made.pop(0), made.pop(0)]
                    if nxt[1] == len(links):
                        done[nxt[0]] = nxt[2]
                    else:
                        after.append(nxt)
                flying = after
            if fresh is not None:
                flying.append(fresh)

        rows = dim // 4
        full = jnp.concatenate([done[i].reshape(-1, 6, rows, LANE) for i in range(len(groups))], axis=0)
        g_up, g_lin = unpack_call(full)
        place = {unit: i for i, unit in enumerate(ORDER)}
        blocks = [full[place[unit], 2:4].reshape(dim // LANE, half, LANE) for unit in range(n_units)]
        mid = n_units // 2
        low, high = jnp.stack(blocks[:mid]), jnp.stack(blocks[mid + 1 :])
        received = swap(jnp.where(core == 0, high, low), 'fsdp', 1)
        own = jnp.where(core == 0, low, high)
        pairs = jnp.where(core == 0, jnp.stack([own, received], axis=1), jnp.stack([received, own], axis=1))
        pairs = pairs.reshape(2 * mid, dim // LANE, half, LANE)
        centre = blocks[mid][None]
        g_down = rows_call(jnp.where(core == 0, jnp.concatenate([pairs, centre]), jnp.concatenate([centre, pairs])))
        return g_up[None], g_lin[None], g_down[None], out

    return jax.shard_map(local_step, mesh=mesh, in_specs=(act_spec, tok_spec, weight_spec, weight_spec, weight_spec), out_specs=(weight_spec, weight_spec, weight_spec, tok_spec), check_vma=False)
```

```python
import functools

import jax
import jax.numpy as jnp
from jax import lax
from jax.experimental import pallas as pl
from jax.experimental.pallas import tpu as pltpu
from jax.sharding import PartitionSpec as P

NORM_EPS = 1e-5
LANE = 128
CHUNKS = ((0, 1, 10, 11), (2, 3, 4, 12, 13, 14), (5, 6, 7, 8, 15, 16, 17, 18, 9))
ORDER = sum(CHUNKS, ())
GROUP = 2
TILE = 512
DN_TILE = 1024
SPLIT = 3
DN_STEP = 256
ALL_VMEM = 67043328
F32 = jnp.float32
BF16 = jnp.bfloat16


def dot(a, b):
    return lax.dot_general(a, b, (((1,), (0,)), ((), ())), preferred_element_type=F32)


def dot_t(a, b):
    return lax.dot_general(a, b, (((1,), (1,)), ((), ())), preferred_element_type=F32)


def sections(chunk):
    even = len(chunk) // GROUP * GROUP
    return [section for section in (chunk[:even], chunk[even:]) if section]


def pack_kernel(up_ref, lin_ref, *outs):
    units = len(ORDER)
    for chunk, out_ref in zip(CHUNKS, outs):
        at = 0
        for section in sections(chunk):
            for ref in (up_ref, lin_ref):
                for unit in section:
                    for x in range(2):
                        out_ref[:, pl.ds(at, LANE)] = ref[:, pl.ds((x * units + unit) * LANE, LANE)]
                        at += LANE


def pack_call(up, lin):
    rows, width = up.shape
    block = rows // 7
    spec = pl.BlockSpec((block, width), lambda i: (i, 0))
    return pl.pallas_call(
        pack_kernel,
        grid=(7,),
        in_specs=[spec, spec],
        out_specs=[pl.BlockSpec((block, 4 * len(chunk) * LANE), lambda i: (i, 0)) for chunk in CHUNKS],
        out_shape=[jax.ShapeDtypeStruct((rows, 4 * len(chunk) * LANE), BF16) for chunk in CHUNKS],
        compiler_params=pltpu.CompilerParams(dimension_semantics=('arbitrary',)),
        name='pack',
    )(up, lin)


def norm_kernel(h_ref, g_ref, n_ref, nt_ref, gt_ref):
    h = h_ref[...].astype(F32)
    normed = (h * lax.rsqrt(jnp.mean(h * h, axis=-1, keepdims=True) + NORM_EPS)).astype(BF16)
    n_ref[...] = normed
    nt_ref[...] = normed.T
    gt_ref[...] = g_ref[...].T


def norm_call(h, grad):
    tokens, dim = h.shape
    tok = pl.BlockSpec((TILE, dim), lambda i: (i, 0))
    tok_t = pl.BlockSpec((dim, TILE), lambda i: (0, i))
    return pl.pallas_call(
        norm_kernel,
        grid=(tokens // TILE,),
        in_specs=[tok, tok],
        out_specs=[tok, tok_t, tok_t],
        out_shape=[jax.ShapeDtypeStruct((tokens, dim), BF16)] + [jax.ShapeDtypeStruct((dim, tokens), BF16)] * 2,
        compiler_params=pltpu.CompilerParams(dimension_semantics=('arbitrary',)),
        cost_estimate=pl.CostEstimate(flops=10**7, bytes_accessed=10 * tokens * dim, transcendentals=0),
        name='norm',
    )(h, grad)


def group_kernel(units, core_ref, n_ref, nt_ref, g_ref, gt_ref, *refs):
    up_ref, lin_ref, blocks = refs[0], refs[1], refs[2 : 2 + 4 * units]
    du_ref, dv_ref, send_ref, keep_ref, acc_up, acc_lin, acc_down, flip, down_ref = refs[-9:]
    step = pl.program_id(0)

    @pl.when(step == 0)
    def _():
        acc_up[...] = jnp.zeros_like(acc_up)
        acc_lin[...] = jnp.zeros_like(acc_lin)
        acc_down[...] = jnp.zeros_like(acc_down)
        half = LANE // 2
        for i in range(4 * units):
            down_ref[pl.ds(i * half, half), :] = blocks[i][...]

    u = dot(n_ref[...], up_ref[...])
    v = dot(n_ref[...], lin_ref[...])
    da = dot_t(g_ref[...], down_ref[...])
    s = jax.nn.sigmoid(u)
    us = u * s
    a = (us * v).astype(BF16)
    du = (da * v * s * (1.0 + u * (1.0 - s))).astype(BF16)
    dv = (da * us).astype(BF16)
    du_ref[...] = du
    dv_ref[...] = dv
    acc_down[...] += dot(gt_ref[...], a)
    acc_up[...] += dot(nt_ref[...], du)
    acc_lin[...] += dot(nt_ref[...], dv)

    @pl.when(step == pl.num_programs(0) - 1)
    def _():
        core = core_ref[0]
        rows = acc_up.shape[0] // 4
        unit_rows = 6 * rows
        for unit in range(units):
            base = unit * unit_rows
            for x in range(2):
                flip[...] = acc_down[:, pl.ds((2 * unit + x) * LANE, LANE)].T
                for out_ref, owner in ((send_ref, 1 - core), (keep_ref, core)):
                    first = pl.multiple_of((2 * x + owner) * rows, 8)
                    for piece in range(2):
                        cols = pl.ds((2 * unit + piece) * LANE, LANE)
                        out_ref[x, pl.ds(base + piece * rows, rows), :] = acc_up[pl.ds(first, rows), cols]
                        out_ref[x, pl.ds(base + (4 + piece) * rows, rows), :] = acc_lin[pl.ds(first, rows), cols]
                    half = LANE // 2
                    for lane in range(flip.shape[1] // LANE):
                        out_ref[x, pl.ds(base + 2 * rows + lane * half, half), :] = flip[pl.ds(pl.multiple_of(owner * half, 8), half), pl.ds(lane * LANE, LANE)]


def chunk_of(unit):
    for index, chunk in enumerate(CHUNKS):
        if unit in chunk:
            return index, chunk


def row_block(unit, x, half):
    index, chunk = chunk_of(unit)
    mid = len(ORDER) // 2
    length = sum(2 if other < mid else 1 for other in chunk if other <= mid)
    core = half if unit == mid else int(unit > mid)
    mates = [other for other in chunk if other != mid and (other > mid) == (unit > mid)]
    place = 2 * len(mates) if unit == mid else 2 * mates.index(unit) + half
    return (2 * x + core) * length + place


def group_call(group, offset, token, normed, normed_t, grad, grad_t, cols, downs, d_up, d_lin):
    tokens, dim = normed.shape
    units = len(group)
    width = 2 * LANE * units
    total = 2 * LANE * len(ORDER)
    packed = units * 6 * (dim // 4)
    tok = pl.BlockSpec((TILE, dim), lambda i, c: (i, 0))
    tok_t = pl.BlockSpec((dim, TILE), lambda i, c: (0, i))
    wide = pl.BlockSpec((TILE, width), lambda i, c: (i, offset // units))
    out = pl.BlockSpec((2, packed, LANE), lambda i, c: (0, 0, 0))
    ins = [token, normed, normed_t, grad, grad_t]
    in_specs = [tok, tok_t, tok, tok_t]
    index, chunk = chunk_of(group[0])
    base = 0
    for section in sections(chunk):
        if group[0] in section:
            break
        base += 2 * len(section)
    place = base + section.index(group[0])
    assert place % units == 0 and len(section) % units == 0
    for at in (place // units, (place + len(section)) // units):
        ins.append(cols[index])
        in_specs.append(pl.BlockSpec((dim, width), lambda i, c, at=at: (0, at)))
    for unit in group:
        for x in range(2):
            for half in range(2):
                ins.append(downs[chunk_of(unit)[0]])
                in_specs.append(pl.BlockSpec((LANE // 2, dim), lambda i, c, at=row_block(unit, x, half): (at, 0)))
    aliases = {}
    if d_up is not None:
        aliases = {len(ins): 0, len(ins) + 1: 1}
        ins += [d_up, d_lin]
        in_specs += [pl.BlockSpec(memory_space=pl.ANY)] * 2
    return pl.pallas_call(
        functools.partial(group_kernel, units),
        grid_spec=pltpu.PrefetchScalarGridSpec(
            num_scalar_prefetch=1,
            grid=(tokens // TILE,),
            in_specs=in_specs,
            out_specs=[wide, wide, out, out],
            scratch_shapes=[pltpu.VMEM((dim, width), F32)] * 3 + [pltpu.VMEM((LANE, dim), F32)] + [pltpu.VMEM((width, dim), BF16)],
        ),
        out_shape=[jax.ShapeDtypeStruct((tokens, total), BF16)] * 2 + [jax.ShapeDtypeStruct((2, packed, LANE), F32)] * 2,
        input_output_aliases=aliases,
        compiler_params=pltpu.CompilerParams(dimension_semantics=('arbitrary',), vmem_limit_bytes=ALL_VMEM),
        cost_estimate=pl.CostEstimate(flops=12 * tokens * dim * width, bytes_accessed=8 * tokens * dim, transcendentals=tokens * width),
        name='group',
    )(*ins)


def advance_kernel(plan, pos_ref, *refs):
    ins, outs = refs[: sum(4 if bit is not None and not gather else 2 for bit, gather in plan)], refs[-sum(1 if gather or bit is None else 2 for bit, gather in plan) :]
    for bit, gather in plan:
        if gather:
            at = pos_ref[bit]
            outs[0][at] = ins[0][...]
            outs[0][1 - at] = ins[1][...]
            ins, outs = ins[2:], outs[1:]
        elif bit is None:
            outs[0][...] = ins[0][...] + ins[1][...]
            ins, outs = ins[2:], outs[1:]
        else:
            outs[0][...] = ins[0][...] + ins[1][...]
            outs[1][...] = ins[2][...] + ins[3][...]
            ins, outs = ins[4:], outs[2:]


def advance_call(pos, plan, pairs):
    ins, in_specs, shapes, out_specs = [pos], [], [], []
    for (bit, gather), (kept, got) in zip(plan, pairs):
        rows = kept.shape[-2] if kept.ndim == 3 else kept.shape[0]
        if gather:
            block = rows // SPLIT
            ins += [kept, got]
            in_specs += [pl.BlockSpec((block, LANE), lambda i, p: (i, 0))] * 2
            shapes.append(jax.ShapeDtypeStruct((2, rows, LANE), F32))
            out_specs.append(pl.BlockSpec((2, block, LANE), lambda i, p: (0, i, 0)))
        elif bit is None:
            block = rows // SPLIT
            ins += [kept, got]
            in_specs += [pl.BlockSpec((block, LANE), lambda i, p: (i, 0))] * 2
            shapes.append(jax.ShapeDtypeStruct((rows, LANE), F32))
            out_specs.append(pl.BlockSpec((block, LANE), lambda i, p: (i, 0)))
        else:
            if kept.ndim == 2:
                rows //= 2
                kept, got = kept.reshape(2, rows, LANE), got.reshape(2, rows, LANE)
            block = rows // SPLIT
            other = pl.BlockSpec((None, block, LANE), lambda i, p, bit=bit: (1 - p[bit], i, 0))
            mine = pl.BlockSpec((None, block, LANE), lambda i, p, bit=bit: (p[bit], i, 0))
            ins += [kept, got, kept, got]
            in_specs += [other, other, mine, mine]
            shapes += [jax.ShapeDtypeStruct((rows, LANE), F32)] * 2
            out_specs += [pl.BlockSpec((block, LANE), lambda i, p: (i, 0))] * 2
    return pl.pallas_call(
        functools.partial(advance_kernel, plan),
        grid_spec=pltpu.PrefetchScalarGridSpec(num_scalar_prefetch=1, grid=(SPLIT,), in_specs=in_specs, out_specs=out_specs),
        out_shape=shapes,
        compiler_params=pltpu.CompilerParams(dimension_semantics=('arbitrary',), vmem_limit_bytes=ALL_VMEM),
        cost_estimate=pl.CostEstimate(flops=10**7, bytes_accessed=2 * 10**7, transcendentals=0),
        name='advance',
    )(*ins)


def unpack_kernel(groups, *refs):
    count = len(groups)
    up_out, lin_out = refs[-2:]
    units = len(ORDER)
    for group, up_ref, lin_ref in zip(groups, refs[:count], refs[count:]):
        for index, unit in enumerate(group):
            for x in range(2):
                cols = pl.ds((x * units + unit) * LANE, LANE)
                up_out[:, cols] = up_ref[index, x]
                lin_out[:, cols] = lin_ref[index, x]


def unpack_call(groups, packed):
    rows = packed[0].shape[2]
    width = 2 * len(ORDER) * LANE
    block = rows // 7
    specs = [pl.BlockSpec((len(group), 2, block, LANE), lambda i, at=at: (0, at, i, 0)) for at in (0, 2) for group in groups]
    return pl.pallas_call(
        functools.partial(unpack_kernel, groups),
        grid=(7,),
        in_specs=specs,
        out_specs=[pl.BlockSpec((block, width), lambda i: (i, 0))] * 2,
        out_shape=[jax.ShapeDtypeStruct((rows, width), F32)] * 2,
        compiler_params=pltpu.CompilerParams(dimension_semantics=('arbitrary',)),
        name='unpack',
    )(*packed, *packed)


def pick_kernel(groups, pos_ref, *refs):
    send_ref, own_ref, mid_ref = refs[-3:]
    low_core = pos_ref[0] == 0
    where = {unit: (ref, index) for group, ref in zip(groups, refs) for index, unit in enumerate(group)}
    mid = len(ORDER) // 2
    for i in range(mid):
        ref, index = where[i]
        low = ref[index].reshape(send_ref.shape[1:])
        ref, index = where[mid + 1 + i]
        high = ref[index].reshape(send_ref.shape[1:])
        send_ref[i] = jnp.where(low_core, high, low)
        own_ref[i] = jnp.where(low_core, low, high)
    ref, index = where[mid]
    mid_ref[...] = ref[index].reshape(mid_ref.shape)


def pick_call(groups, pos, packed):
    rows = packed[0].shape[2]
    mid = len(ORDER) // 2
    one = (2 * rows, LANE)
    specs = [pl.BlockSpec((len(group), 2, rows, LANE), lambda i, p: (0, 1, 0, 0)) for group in groups]
    return pl.pallas_call(
        functools.partial(pick_kernel, groups),
        grid_spec=pltpu.PrefetchScalarGridSpec(
            num_scalar_prefetch=1,
            grid=(1,),
            in_specs=specs,
            out_specs=[pl.BlockSpec((mid,) + one, lambda i, p: (0, 0, 0))] * 2 + [pl.BlockSpec(one, lambda i, p: (0, 0))],
        ),
        out_shape=[jax.ShapeDtypeStruct((mid,) + one, F32)] * 2 + [jax.ShapeDtypeStruct(one, F32)],
        compiler_params=pltpu.CompilerParams(dimension_semantics=('arbitrary',)),
        name='pick',
    )(pos, *packed)


def rows_kernel(pos_ref, own_ref, got_ref, mid_ref, out_ref):
    core = pos_ref[0]
    half = LANE // 2
    count = own_ref.shape[0]
    for lane in range(own_ref.shape[1] // half):
        cols = pl.ds(lane * LANE, LANE)
        part = pl.ds(lane * half, half)
        out_ref[pl.ds(pl.multiple_of((1 - core) * count * LANE, 8), half), cols] = mid_ref[part, :]
        for i in range(count):
            own, got = own_ref[i, part, :], got_ref[i, part, :]
            first = pl.multiple_of(core * half + i * LANE, 8)
            out_ref[pl.ds(first, half), cols] = jnp.where(core == 0, own, got)
            out_ref[pl.ds(pl.multiple_of(first + half, 8), half), cols] = jnp.where(core == 0, got, own)


def rows_call(pos, own, got, mid):
    count, rows, _ = own.shape
    shape = ((2 * count + 1) * LANE // 2, rows * 2)
    whole = pl.BlockSpec(own.shape, lambda i, p: (0, 0, 0))
    return pl.pallas_call(
        rows_kernel,
        grid_spec=pltpu.PrefetchScalarGridSpec(
            num_scalar_prefetch=1,
            grid=(1,),
            in_specs=[whole, whole, pl.BlockSpec(mid.shape, lambda i, p: (0, 0))],
            out_specs=pl.BlockSpec(shape, lambda i, p: (0, 0)),
        ),
        out_shape=jax.ShapeDtypeStruct(shape, F32),
        compiler_params=pltpu.CompilerParams(dimension_semantics=('arbitrary',)),
        name='rows',
    )(pos, own, got, mid)


def input_kernel(token_ref, du_ref, dv_ref, *refs):
    weights, (h_ref, g_ref), out_ref = refs[: len(CHUNKS)], refs[len(CHUNKS) : len(CHUNKS) + 2], refs[-1]
    dn = None
    first = 0
    for chunk, ref in zip(CHUNKS, weights):
        at = 0
        for section in sections(chunk):
            size = 2 * LANE * len(section)
            cols = pl.ds(first, size)
            part = dot_t(du_ref[:, cols], ref[:, pl.ds(at, size)]) + dot_t(dv_ref[:, cols], ref[:, pl.ds(at + size, size)])
            dn = part if dn is None else dn + part
            first += size
            at += 2 * size
    h = h_ref[...].astype(F32)
    inv = lax.rsqrt(jnp.mean(h * h, axis=-1, keepdims=True) + NORM_EPS)
    y = h * inv
    d_h = inv * (dn - y * jnp.mean(dn * y, axis=-1, keepdims=True))
    out_ref[...] = (g_ref[...].astype(F32) + d_h).astype(BF16)


def input_call(part, token, d_up, d_lin, cols, h, grad, prev):
    tokens, dim = h.shape
    steps = DN_TILE // DN_STEP
    act = pl.BlockSpec((DN_STEP, d_up.shape[1]), lambda k, c: (part * steps + k, 0))
    tok = pl.BlockSpec((DN_STEP, dim), lambda k, c: (part * steps + k, 0))
    ins = [token, d_up, d_lin, *cols, h, grad]
    in_specs = [act, act] + [pl.BlockSpec(w.shape, lambda k, c: (0, 0), pipeline_mode=pl.Buffered(1)) for w in cols] + [tok, tok]
    aliases = {}
    if prev is not None:
        aliases = {len(ins): 0}
        ins.append(prev)
        in_specs.append(pl.BlockSpec(memory_space=pl.ANY))
    return pl.pallas_call(
        input_kernel,
        grid_spec=pltpu.PrefetchScalarGridSpec(num_scalar_prefetch=1, grid=(steps,), in_specs=in_specs, out_specs=tok),
        out_shape=jax.ShapeDtypeStruct((tokens, dim), BF16),
        input_output_aliases=aliases,
        compiler_params=pltpu.CompilerParams(dimension_semantics=('arbitrary',), vmem_limit_bytes=ALL_VMEM),
        cost_estimate=pl.CostEstimate(flops=4 * DN_TILE * dim * d_up.shape[1], bytes_accessed=4 * DN_TILE * d_up.shape[1], transcendentals=0),
        name='input_grad',
    )(*ins)


def solution(mesh):
    tok_spec = P(('replica', 'fsdp'), None)
    act_spec = P(None, ('replica', 'fsdp'), None)
    weight_spec = P(None, 'fsdp', None)
    n_fsdp, n_rep = mesh.shape['fsdp'], mesh.shape['replica']

    def swap(value, axis, bit):
        size = n_fsdp if axis == 'fsdp' else n_rep
        return lax.ppermute(value, axis, [(i, i ^ bit) for i in range(size)])

    def local_step(block_in, grad_out, w_up, w_lin, w_down):
        h = block_in[0]
        dim, ff = h.shape[1], w_up.shape[2]
        n_units = len(ORDER)
        fsdp, rep = lax.axis_index('fsdp'), lax.axis_index('replica')
        core = fsdp % 2
        pos = jnp.stack([core, fsdp // 2, rep % 2, (rep // 2) % 2, rep // 4]).astype(jnp.int32)

        gather = lambda w: lax.all_gather(w, 'fsdp', axis=0, tiled=True)
        half = LANE // 2
        rolled = jnp.concatenate([w_down[0], w_down[0][:half]], axis=0)
        cols, downs = [], []
        start = 0
        for chunk, both in zip(CHUNKS, pack_call(w_up[0], w_lin[0])):
            length = half * len(chunk)
            cols.append(gather(both))
            downs.append(gather(lax.dynamic_slice_in_dim(rolled, start + core * half, length, 0)))
            start += length

        normed, normed_t, grad_t = norm_call(h, grad_out)

        groups = []
        for chunk in CHUNKS:
            groups += [chunk[i : i + GROUP] for i in range(0, len(chunk), GROUP)]
        links = (('fsdp', 1), ('fsdp', 2), ('replica', 1), ('replica', 2), ('replica', 4), ('replica', 4), ('replica', 2), ('replica', 1))
        plan_of = ((1, False), (2, False), (3, False), (4, False), (None, False), (4, True), (3, True), (2, True))

        d_up = d_lin = out = None
        parts = h.shape[0] // DN_TILE
        flying, done = [], {}
        slot = part = offset = 0
        while slot < len(groups) or part < parts or flying:
            token, sends, out = lax.optimization_barrier((pos, [item[2] for item in flying], out))
            got = [swap(value, *links[item[1]]) for value, item in zip(sends, flying)]
            fresh = None
            if slot < len(groups):
                d_up, d_lin, send, keep = group_call(groups[slot], offset, token, normed, normed_t, grad_out, grad_t, cols, downs, d_up, d_lin)
                fresh = [slot, 0, send, keep]
                offset += len(groups[slot])
                slot += 1
            elif part < parts:
                out = input_call(part, token, d_up, d_lin, cols, h, grad_out, out)
                part += 1
            if flying:
                plan = tuple(plan_of[item[1]] for item in flying)
                made = list(advance_call(pos, plan, [(item[3], value) for item, value in zip(flying, got)]))
                after = []
                for (bit, joined), item in zip(plan, flying):
                    if joined or bit is None:
                        value = made.pop(0)
                        value = value.reshape(-1, LANE)
                        nxt = [item[0], item[1] + 1, value, value]
                    else:
                        nxt = [item[0], item[1] + 1, made.pop(0), made.pop(0)]
                    if nxt[1] == len(links):
                        done[nxt[0]] = nxt[2]
                    else:
                        after.append(nxt)
                flying = after
            if fresh is not None:
                flying.append(fresh)

        packed = [done[i].reshape(-1, 6, dim // 4, LANE) for i in range(len(groups))]
        send, own, centre = pick_call(groups, pos, packed)
        received = swap(send, 'fsdp', 1)
        g_up, g_lin = unpack_call(groups, packed)
        g_down = rows_call(pos, own, received, centre)
        return g_up[None], g_lin[None], g_down[None], out

    return jax.shard_map(local_step, mesh=mesh, in_specs=(act_spec, tok_spec, weight_spec, weight_spec, weight_spec), out_specs=(weight_spec, weight_spec, weight_spec, tok_spec), check_vma=False)
```

```python
import functools

import jax
import jax.numpy as jnp
from jax import lax
from jax.experimental import pallas as pl
from jax.experimental.pallas import tpu as pltpu
from jax.sharding import PartitionSpec as P

NORM_EPS = 1e-5
LANE = 128
CHUNKS = ((0, 1, 10, 11), (2, 3, 4, 12, 13, 14), (5, 6, 7, 8, 15, 16, 17, 18, 9))
ORDER = sum(CHUNKS, ())
GROUP = 2
TILE = 1024
DN_TILE = 1024
SPLIT = 1
DN_STEP = 256
ALL_VMEM = 67043328
F32 = jnp.float32
BF16 = jnp.bfloat16


def dot(a, b):
    return lax.dot_general(a, b, (((1,), (0,)), ((), ())), preferred_element_type=F32)


def dot_t(a, b):
    return lax.dot_general(a, b, (((1,), (1,)), ((), ())), preferred_element_type=F32)


def sections(chunk):
    even = len(chunk) // GROUP * GROUP
    return [section for section in (chunk[:even], chunk[even:]) if section]


def pack_kernel(up_ref, lin_ref, *outs):
    units = len(ORDER)
    for chunk, out_ref in zip(CHUNKS, outs):
        at = 0
        for section in sections(chunk):
            for ref in (up_ref, lin_ref):
                for unit in section:
                    for x in range(2):
                        out_ref[:, pl.ds(at, LANE)] = ref[:, pl.ds((x * units + unit) * LANE, LANE)]
                        at += LANE


def pack_call(up, lin):
    rows, width = up.shape
    block = rows // 7
    spec = pl.BlockSpec((block, width), lambda i: (i, 0))
    return pl.pallas_call(
        pack_kernel,
        grid=(7,),
        in_specs=[spec, spec],
        out_specs=[pl.BlockSpec((block, 4 * len(chunk) * LANE), lambda i: (i, 0)) for chunk in CHUNKS],
        out_shape=[jax.ShapeDtypeStruct((rows, 4 * len(chunk) * LANE), BF16) for chunk in CHUNKS],
        compiler_params=pltpu.CompilerParams(dimension_semantics=('arbitrary',)),
        name='pack',
    )(up, lin)


def norm_kernel(h_ref, g_ref, n_ref, nt_ref, gt_ref):
    h = h_ref[...].astype(F32)
    normed = (h * lax.rsqrt(jnp.mean(h * h, axis=-1, keepdims=True) + NORM_EPS)).astype(BF16)
    n_ref[...] = normed
    nt_ref[...] = normed.T
    gt_ref[...] = g_ref[...].T


def norm_call(h, grad):
    tokens, dim = h.shape
    tok = pl.BlockSpec((TILE, dim), lambda i: (i, 0))
    tok_t = pl.BlockSpec((dim, TILE), lambda i: (0, i))
    return pl.pallas_call(
        norm_kernel,
        grid=(tokens // TILE,),
        in_specs=[tok, tok],
        out_specs=[tok, tok_t, tok_t],
        out_shape=[jax.ShapeDtypeStruct((tokens, dim), BF16)] + [jax.ShapeDtypeStruct((dim, tokens), BF16)] * 2,
        compiler_params=pltpu.CompilerParams(dimension_semantics=('arbitrary',)),
        cost_estimate=pl.CostEstimate(flops=10**7, bytes_accessed=10 * tokens * dim, transcendentals=0),
        name='norm',
    )(h, grad)


def group_kernel(units, core_ref, n_ref, nt_ref, g_ref, gt_ref, *refs):
    up_ref, lin_ref, blocks = refs[0], refs[1], refs[2 : 2 + 4 * units]
    du_ref, dv_ref, send_ref, keep_ref, acc_up, acc_lin, acc_down, flip, down_ref = refs[-9:]
    step = pl.program_id(0)

    @pl.when(step == 0)
    def _():
        acc_up[...] = jnp.zeros_like(acc_up)
        acc_lin[...] = jnp.zeros_like(acc_lin)
        acc_down[...] = jnp.zeros_like(acc_down)
        half = LANE // 2
        for i in range(4 * units):
            down_ref[pl.ds(i * half, half), :] = blocks[i][...]

    u = dot(n_ref[...], up_ref[...])
    v = dot(n_ref[...], lin_ref[...])
    da = dot_t(g_ref[...], down_ref[...])
    s = jax.nn.sigmoid(u)
    us = u * s
    a = (us * v).astype(BF16)
    du = (da * v * s * (1.0 + u * (1.0 - s))).astype(BF16)
    dv = (da * us).astype(BF16)
    du_ref[...] = du
    dv_ref[...] = dv
    acc_down[...] += dot(gt_ref[...], a)
    acc_up[...] += dot(nt_ref[...], du)
    acc_lin[...] += dot(nt_ref[...], dv)

    @pl.when(step == pl.num_programs(0) - 1)
    def _():
        core = core_ref[0]
        rows = acc_up.shape[0] // 4
        unit_rows = 6 * rows
        for unit in range(units):
            base = unit * unit_rows
            for x in range(2):
                flip[...] = acc_down[:, pl.ds((2 * unit + x) * LANE, LANE)].T
                for out_ref, owner in ((send_ref, 1 - core), (keep_ref, core)):
                    first = pl.multiple_of((2 * x + owner) * rows, 8)
                    for piece in range(2):
                        cols = pl.ds((2 * unit + piece) * LANE, LANE)
                        out_ref[x, pl.ds(base + piece * rows, rows), :] = acc_up[pl.ds(first, rows), cols]
                        out_ref[x, pl.ds(base + (4 + piece) * rows, rows), :] = acc_lin[pl.ds(first, rows), cols]
                    half = LANE // 2
                    for lane in range(flip.shape[1] // LANE):
                        out_ref[x, pl.ds(base + 2 * rows + lane * half, half), :] = flip[pl.ds(pl.multiple_of(owner * half, 8), half), pl.ds(lane * LANE, LANE)]


def chunk_of(unit):
    for index, chunk in enumerate(CHUNKS):
        if unit in chunk:
            return index, chunk


def row_block(unit, x, half):
    index, chunk = chunk_of(unit)
    mid = len(ORDER) // 2
    length = sum(2 if other < mid else 1 for other in chunk if other <= mid)
    core = half if unit == mid else int(unit > mid)
    mates = [other for other in chunk if other != mid and (other > mid) == (unit > mid)]
    place = 2 * len(mates) if unit == mid else 2 * mates.index(unit) + half
    return (2 * x + core) * length + place


def group_call(group, offset, token, normed, normed_t, grad, grad_t, cols, downs, d_up, d_lin):
    tokens, dim = normed.shape
    units = len(group)
    width = 2 * LANE * units
    total = 2 * LANE * len(ORDER)
    packed = units * 6 * (dim // 4)
    tok = pl.BlockSpec((TILE, dim), lambda i, c: (i, 0))
    tok_t = pl.BlockSpec((dim, TILE), lambda i, c: (0, i))
    wide = pl.BlockSpec((TILE, width), lambda i, c: (i, offset // units))
    out = pl.BlockSpec((2, packed, LANE), lambda i, c: (0, 0, 0))
    ins = [token, normed, normed_t, grad, grad_t]
    in_specs = [tok, tok_t, tok, tok_t]
    index, chunk = chunk_of(group[0])
    base = 0
    for section in sections(chunk):
        if group[0] in section:
            break
        base += 2 * len(section)
    place = base + section.index(group[0])
    assert place % units == 0 and len(section) % units == 0
    for at in (place // units, (place + len(section)) // units):
        ins.append(cols[index])
        in_specs.append(pl.BlockSpec((dim, width), lambda i, c, at=at: (0, at)))
    for unit in group:
        for x in range(2):
            for half in range(2):
                ins.append(downs[chunk_of(unit)[0]])
                in_specs.append(pl.BlockSpec((LANE // 2, dim), lambda i, c, at=row_block(unit, x, half): (at, 0)))
    aliases = {}
    if d_up is not None:
        aliases = {len(ins): 0, len(ins) + 1: 1}
        ins += [d_up, d_lin]
        in_specs += [pl.BlockSpec(memory_space=pl.ANY)] * 2
    return pl.pallas_call(
        functools.partial(group_kernel, units),
        grid_spec=pltpu.PrefetchScalarGridSpec(
            num_scalar_prefetch=1,
            grid=(tokens // TILE,),
            in_specs=in_specs,
            out_specs=[wide, wide, out, out],
            scratch_shapes=[pltpu.VMEM((dim, width), F32)] * 3 + [pltpu.VMEM((LANE, dim), F32)] + [pltpu.VMEM((width, dim), BF16)],
        ),
        out_shape=[jax.ShapeDtypeStruct((tokens, total), BF16)] * 2 + [jax.ShapeDtypeStruct((2, packed, LANE), F32)] * 2,
        input_output_aliases=aliases,
        compiler_params=pltpu.CompilerParams(dimension_semantics=('arbitrary',), vmem_limit_bytes=ALL_VMEM),
        cost_estimate=pl.CostEstimate(flops=12 * tokens * dim * width, bytes_accessed=8 * tokens * dim, transcendentals=tokens * width),
        name='group',
    )(*ins)


def advance_kernel(plan, pos_ref, *refs):
    ins, outs = refs[: sum(4 if bit is not None and not gather else 2 for bit, gather in plan)], refs[-sum(1 if gather or bit is None else 2 for bit, gather in plan) :]
    for bit, gather in plan:
        if gather:
            at = pos_ref[bit]
            outs[0][at] = ins[0][...]
            outs[0][1 - at] = ins[1][...]
            ins, outs = ins[2:], outs[1:]
        elif bit is None:
            outs[0][...] = ins[0][...] + ins[1][...]
            ins, outs = ins[2:], outs[1:]
        else:
            outs[0][...] = ins[0][...] + ins[1][...]
            outs[1][...] = ins[2][...] + ins[3][...]
            ins, outs = ins[4:], outs[2:]


def advance_call(pos, plan, pairs):
    ins, in_specs, shapes, out_specs = [pos], [], [], []
    for (bit, gather), (kept, got) in zip(plan, pairs):
        rows = kept.shape[-2] if kept.ndim == 3 else kept.shape[0]
        if gather:
            block = rows // SPLIT
            ins += [kept, got]
            in_specs += [pl.BlockSpec((block, LANE), lambda i, p: (i, 0))] * 2
            shapes.append(jax.ShapeDtypeStruct((2, rows, LANE), F32))
            out_specs.append(pl.BlockSpec((2, block, LANE), lambda i, p: (0, i, 0)))
        elif bit is None:
            block = rows // SPLIT
            ins += [kept, got]
            in_specs += [pl.BlockSpec((block, LANE), lambda i, p: (i, 0))] * 2
            shapes.append(jax.ShapeDtypeStruct((rows, LANE), F32))
            out_specs.append(pl.BlockSpec((block, LANE), lambda i, p: (i, 0)))
        else:
            if kept.ndim == 2:
                rows //= 2
                kept, got = kept.reshape(2, rows, LANE), got.reshape(2, rows, LANE)
            block = rows // SPLIT
            other = pl.BlockSpec((None, block, LANE), lambda i, p, bit=bit: (1 - p[bit], i, 0))
            mine = pl.BlockSpec((None, block, LANE), lambda i, p, bit=bit: (p[bit], i, 0))
            ins += [kept, got, kept, got]
            in_specs += [other, other, mine, mine]
            shapes += [jax.ShapeDtypeStruct((rows, LANE), F32)] * 2
            out_specs += [pl.BlockSpec((block, LANE), lambda i, p: (i, 0))] * 2
    return pl.pallas_call(
        functools.partial(advance_kernel, plan),
        grid_spec=pltpu.PrefetchScalarGridSpec(num_scalar_prefetch=1, grid=(SPLIT,), in_specs=in_specs, out_specs=out_specs),
        out_shape=shapes,
        compiler_params=pltpu.CompilerParams(dimension_semantics=('arbitrary',), vmem_limit_bytes=ALL_VMEM),
        cost_estimate=pl.CostEstimate(flops=10**7, bytes_accessed=2 * 10**7, transcendentals=0),
        name='advance',
    )(*ins)


def unpack_kernel(groups, *refs):
    count = len(groups)
    up_out, lin_out = refs[-2:]
    units = len(ORDER)
    for group, up_ref, lin_ref in zip(groups, refs[:count], refs[count:]):
        for index, unit in enumerate(group):
            for x in range(2):
                cols = pl.ds((x * units + unit) * LANE, LANE)
                up_out[:, cols] = up_ref[index, x]
                lin_out[:, cols] = lin_ref[index, x]


def unpack_call(groups, packed):
    rows = packed[0].shape[2]
    width = 2 * len(ORDER) * LANE
    block = rows // 7
    specs = [pl.BlockSpec((len(group), 2, block, LANE), lambda i, at=at: (0, at, i, 0)) for at in (0, 2) for group in groups]
    return pl.pallas_call(
        functools.partial(unpack_kernel, groups),
        grid=(7,),
        in_specs=specs,
        out_specs=[pl.BlockSpec((block, width), lambda i: (i, 0))] * 2,
        out_shape=[jax.ShapeDtypeStruct((rows, width), F32)] * 2,
        compiler_params=pltpu.CompilerParams(dimension_semantics=('arbitrary',)),
        name='unpack',
    )(*packed, *packed)


def pick_kernel(groups, pos_ref, *refs):
    send_ref, own_ref, mid_ref = refs[-3:]
    low_core = pos_ref[0] == 0
    where = {unit: (ref, index) for group, ref in zip(groups, refs) for index, unit in enumerate(group)}
    mid = len(ORDER) // 2
    for i in range(mid):
        ref, index = where[i]
        low = ref[index].reshape(send_ref.shape[1:])
        ref, index = where[mid + 1 + i]
        high = ref[index].reshape(send_ref.shape[1:])
        send_ref[i] = jnp.where(low_core, high, low)
        own_ref[i] = jnp.where(low_core, low, high)
    ref, index = where[mid]
    mid_ref[...] = ref[index].reshape(mid_ref.shape)


def pick_call(groups, pos, packed):
    rows = packed[0].shape[2]
    mid = len(ORDER) // 2
    one = (2 * rows, LANE)
    specs = [pl.BlockSpec((len(group), 2, rows, LANE), lambda i, p: (0, 1, 0, 0)) for group in groups]
    return pl.pallas_call(
        functools.partial(pick_kernel, groups),
        grid_spec=pltpu.PrefetchScalarGridSpec(
            num_scalar_prefetch=1,
            grid=(1,),
            in_specs=specs,
            out_specs=[pl.BlockSpec((mid,) + one, lambda i, p: (0, 0, 0))] * 2 + [pl.BlockSpec(one, lambda i, p: (0, 0))],
        ),
        out_shape=[jax.ShapeDtypeStruct((mid,) + one, F32)] * 2 + [jax.ShapeDtypeStruct(one, F32)],
        compiler_params=pltpu.CompilerParams(dimension_semantics=('arbitrary',)),
        name='pick',
    )(pos, *packed)


def rows_kernel(pos_ref, own_ref, got_ref, mid_ref, out_ref):
    core = pos_ref[0]
    half = LANE // 2
    count = own_ref.shape[0]
    for lane in range(own_ref.shape[1] // half):
        cols = pl.ds(lane * LANE, LANE)
        part = pl.ds(lane * half, half)
        out_ref[pl.ds(pl.multiple_of((1 - core) * count * LANE, 8), half), cols] = mid_ref[part, :]
        for i in range(count):
            own, got = own_ref[i, part, :], got_ref[i, part, :]
            first = pl.multiple_of(core * half + i * LANE, 8)
            out_ref[pl.ds(first, half), cols] = jnp.where(core == 0, own, got)
            out_ref[pl.ds(pl.multiple_of(first + half, 8), half), cols] = jnp.where(core == 0, got, own)


def rows_call(pos, own, got, mid):
    count, rows, _ = own.shape
    shape = ((2 * count + 1) * LANE // 2, rows * 2)
    whole = pl.BlockSpec(own.shape, lambda i, p: (0, 0, 0))
    return pl.pallas_call(
        rows_kernel,
        grid_spec=pltpu.PrefetchScalarGridSpec(
            num_scalar_prefetch=1,
            grid=(1,),
            in_specs=[whole, whole, pl.BlockSpec(mid.shape, lambda i, p: (0, 0))],
            out_specs=pl.BlockSpec(shape, lambda i, p: (0, 0)),
        ),
        out_shape=jax.ShapeDtypeStruct(shape, F32),
        compiler_params=pltpu.CompilerParams(dimension_semantics=('arbitrary',)),
        name='rows',
    )(pos, own, got, mid)


def input_kernel(token_ref, du_ref, dv_ref, *refs):
    weights, (h_ref, g_ref), out_ref = refs[: len(CHUNKS)], refs[len(CHUNKS) : len(CHUNKS) + 2], refs[-1]
    dn = None
    first = 0
    for chunk, ref in zip(CHUNKS, weights):
        at = 0
        for section in sections(chunk):
            size = 2 * LANE * len(section)
            cols = pl.ds(first, size)
            part = dot_t(du_ref[:, cols], ref[:, pl.ds(at, size)]) + dot_t(dv_ref[:, cols], ref[:, pl.ds(at + size, size)])
            dn = part if dn is None else dn + part
            first += size
            at += 2 * size
    h = h_ref[...].astype(F32)
    inv = lax.rsqrt(jnp.mean(h * h, axis=-1, keepdims=True) + NORM_EPS)
    y = h * inv
    d_h = inv * (dn - y * jnp.mean(dn * y, axis=-1, keepdims=True))
    out_ref[...] = (g_ref[...].astype(F32) + d_h).astype(BF16)


def input_call(part, token, d_up, d_lin, cols, h, grad, prev):
    tokens, dim = h.shape
    steps = DN_TILE // DN_STEP
    act = pl.BlockSpec((DN_STEP, d_up.shape[1]), lambda k, c: (part * steps + k, 0))
    tok = pl.BlockSpec((DN_STEP, dim), lambda k, c: (part * steps + k, 0))
    ins = [token, d_up, d_lin, *cols, h, grad]
    in_specs = [act, act] + [pl.BlockSpec(w.shape, lambda k, c: (0, 0), pipeline_mode=pl.Buffered(1)) for w in cols] + [tok, tok]
    aliases = {}
    if prev is not None:
        aliases = {len(ins): 0}
        ins.append(prev)
        in_specs.append(pl.BlockSpec(memory_space=pl.ANY))
    return pl.pallas_call(
        input_kernel,
        grid_spec=pltpu.PrefetchScalarGridSpec(num_scalar_prefetch=1, grid=(steps,), in_specs=in_specs, out_specs=tok),
        out_shape=jax.ShapeDtypeStruct((tokens, dim), BF16),
        input_output_aliases=aliases,
        compiler_params=pltpu.CompilerParams(dimension_semantics=('arbitrary',), vmem_limit_bytes=ALL_VMEM),
        cost_estimate=pl.CostEstimate(flops=4 * DN_TILE * dim * d_up.shape[1], bytes_accessed=4 * DN_TILE * d_up.shape[1], transcendentals=0),
        name='input_grad',
    )(*ins)


def solution(mesh):
    tok_spec = P(('replica', 'fsdp'), None)
    act_spec = P(None, ('replica', 'fsdp'), None)
    weight_spec = P(None, 'fsdp', None)
    n_fsdp, n_rep = mesh.shape['fsdp'], mesh.shape['replica']

    def swap(value, axis, bit):
        size = n_fsdp if axis == 'fsdp' else n_rep
        return lax.ppermute(value, axis, [(i, i ^ bit) for i in range(size)])

    def local_step(block_in, grad_out, w_up, w_lin, w_down):
        h = block_in[0]
        dim, ff = h.shape[1], w_up.shape[2]
        n_units = len(ORDER)
        fsdp, rep = lax.axis_index('fsdp'), lax.axis_index('replica')
        core = fsdp % 2
        pos = jnp.stack([core, fsdp // 2, rep % 2, (rep // 2) % 2, rep // 4]).astype(jnp.int32)

        gather = lambda w: lax.all_gather(w, 'fsdp', axis=0, tiled=True)
        half = LANE // 2
        rolled = jnp.concatenate([w_down[0], w_down[0][:half]], axis=0)
        cols, downs = [], []
        start = 0
        for chunk, both in zip(CHUNKS, pack_call(w_up[0], w_lin[0])):
            length = half * len(chunk)
            cols.append(gather(both))
            downs.append(gather(lax.dynamic_slice_in_dim(rolled, start + core * half, length, 0)))
            start += length

        normed, normed_t, grad_t = norm_call(h, grad_out)

        groups = []
        for chunk in CHUNKS:
            groups += [chunk[i : i + GROUP] for i in range(0, len(chunk), GROUP)]
        links = (('fsdp', 1), ('fsdp', 2), ('replica', 1), ('replica', 2), ('replica', 4), ('replica', 4), ('replica', 2), ('replica', 1))
        plan_of = ((1, False), (2, False), (3, False), (4, False), (None, False), (4, True), (3, True), (2, True))

        d_up = d_lin = out = None
        parts = h.shape[0] // DN_TILE
        flying, done = [], {}
        slot = part = offset = 0
        while slot < len(groups) or part < parts or flying:
            token, sends, out = lax.optimization_barrier((pos, [item[2] for item in flying], out))
            got = [swap(value, *links[item[1]]) for value, item in zip(sends, flying)]
            fresh = None
            if slot < len(groups):
                d_up, d_lin, send, keep = group_call(groups[slot], offset, token, normed, normed_t, grad_out, grad_t, cols, downs, d_up, d_lin)
                fresh = [slot, 0, send, keep]
                offset += len(groups[slot])
                slot += 1
            elif part < parts:
                out = input_call(part, token, d_up, d_lin, cols, h, grad_out, out)
                part += 1
            if flying:
                plan = tuple(plan_of[item[1]] for item in flying)
                made = list(advance_call(pos, plan, [(item[3], value) for item, value in zip(flying, got)]))
                after = []
                for (bit, joined), item in zip(plan, flying):
                    if joined or bit is None:
                        value = made.pop(0)
                        value = value.reshape(-1, LANE)
                        nxt = [item[0], item[1] + 1, value, value]
                    else:
                        nxt = [item[0], item[1] + 1, made.pop(0), made.pop(0)]
                    if nxt[1] == len(links):
                        done[nxt[0]] = nxt[2]
                    else:
                        after.append(nxt)
                flying = after
            if fresh is not None:
                flying.append(fresh)

        packed = [done[i].reshape(-1, 6, dim // 4, LANE) for i in range(len(groups))]
        send, own, centre = pick_call(groups, pos, packed)
        received = swap(send, 'fsdp', 1)
        g_up, g_lin = unpack_call(groups, packed)
        g_down = rows_call(pos, own, received, centre)
        return g_up[None], g_lin[None], g_down[None], out

    return jax.shard_map(local_step, mesh=mesh, in_specs=(act_spec, tok_spec, weight_spec, weight_spec, weight_spec), out_specs=(weight_spec, weight_spec, weight_spec, tok_spec), check_vma=False)
```
